32 devices in a mesh: owner: 4 (over y, x), rows: 8 (over z, core).
Axes of the slice: x: 2, y: 2, z: 4, core: 2. Of those that a mesh axis runs over, the one named last changes fastest.
Arguments:
- w_gate: float32 [64, 2048, 1024], P('owner', 'rows'), may hold values from -0.1875 to 0.1875
- avg_gate: bfloat16 [64, 2048, 1024], P('owner', 'rows'), may hold values from -0.0625 to 0.0625
- w_up: float32 [64, 2048, 1024], P('owner', 'rows'), may hold values from -0.1875 to 0.1875
- avg_up: bfloat16 [64, 2048, 1024], P('owner', 'rows'), may hold values from -0.0625 to 0.0625
- w_down: float32 [64, 1024, 2048], P('owner', None, 'rows'), may hold values from -0.25 to 0.25
- avg_down: bfloat16 [64, 1024, 2048], P('owner', None, 'rows'), may hold values from -0.09375 to 0.09375
- router_weight: float32 [2048, 64], P('rows', 'owner'), may hold values from -0.125 to 0.125
- router_gain: float32 [2048], P('rows'), may hold values from 0.25 to 1.75
Outputs:
- serve_gate: bfloat16 [64, 2048, 1024], P('owner', None, 'rows')
- serve_up: bfloat16 [64, 2048, 1024], P('owner', None, 'rows')
- serve_down: bfloat16 [64, 1024, 2048], P('owner', 'rows')
- scale_gate: float32 [64, 1024], P('owner', 'rows')
- scale_up: float32 [64, 1024], P('owner', 'rows')
- scale_down: float32 [64, 1024], P('owner', 'rows')
- serve_router: bfloat16 [2048, 64], replicated
The draws below stay inside these ranges and needn't reach their ends.
All inputs are finite; a program needn't handle non-finite values.
Results may differ from the reference program's by a relative error of at most 0.0015.
Values may be sent and summed in bfloat16 or wider, within the bound.
A program may use at most 192 MiB of HBM per device.

```python
import jax
import jax.numpy as jnp
from jax import lax

EXPERTS = 64
D_MODEL = 2048
D_EXPERT = 1024


def raised(drawn, stream_key, source, target, shards_of, factor):
    owner, partner = [(jnp.arange(drawn.shape[position]) // (drawn.shape[position] // shards_of)).reshape([-1 if axis == position else 1 for axis in range(drawn.ndim)]) for position in (source, target)]
    chosen = jax.random.permutation(stream_key, shards_of)[partner]
    strong = (owner == chosen) | (owner == (partner + shards_of // 2) % shards_of)
    return jnp.where(strong, factor * drawn, drawn)


def shard_levels(key, dims, shards, smallest, top_value):
    factor_of = 1.0
    for position, blocks in shards:
        draws = jax.random.uniform(jax.random.fold_in(jax.random.fold_in(key, 6), position), (blocks,), jnp.float32, smallest / len(shards), top_value / len(shards))
        factor_of = factor_of * jnp.repeat(jnp.exp(draws), dims[position] // blocks).reshape((-1,) + (1,) * (len(dims) - 1 - position))
    return factor_of


def centred(own_key, dims, spread, limit, pieces=(), held_as=jnp.bfloat16):
    factor_of = shard_levels(own_key, dims, pieces, -0.22, 0.18) if pieces else 1.0
    entries = jax.random.normal(own_key, dims, jnp.float32) * spread * factor_of
    return jnp.minimum(jnp.maximum(entries, -limit), limit).astype(held_as)


def noise_with(stream_key, shape, deviation, limit, cuts, heavy, dtype=jnp.bfloat16):
    result = deviation * jax.random.normal(stream_key, shape, jnp.float32)
    if cuts:
        result = result * shard_levels(stream_key, shape, cuts, -0.22, 0.18)
    return jnp.clip(raised(result, jax.random.fold_in(stream_key, 3), *heavy), -limit, limit).astype(dtype)


def setup_inputs(seed: int = 0) -> dict:
    streams_of = jax.random.split(jax.random.key(seed), 9)
    w_gate = noise_with(streams_of[0], (EXPERTS, D_MODEL, D_EXPERT), D_MODEL ** -0.5, 0.1875, ((0, 4), (1, 8)), (1, 2, 8, 2.0), jnp.float32)
    avg_gate = centred(streams_of[1], (EXPERTS, D_MODEL, D_EXPERT), (D_MODEL * 4) ** -0.5, 0.0625, ((0, 4), (1, 8)))
    w_up = noise_with(streams_of[2], (EXPERTS, D_MODEL, D_EXPERT), D_MODEL ** -0.5, 0.1875, ((0, 4), (1, 8)), (1, 2, 8, 2.0), jnp.float32)
    avg_up = centred(streams_of[3], (EXPERTS, D_MODEL, D_EXPERT), (D_MODEL * 4) ** -0.5, 0.0625, ((0, 4), (1, 8)))
    w_down = noise_with(streams_of[4], (EXPERTS, D_EXPERT, D_MODEL), D_EXPERT ** -0.5, 0.25, ((0, 4), (2, 8)), (2, 1, 8, 2.0), jnp.float32)
    avg_down = centred(streams_of[5], (EXPERTS, D_EXPERT, D_MODEL), (D_EXPERT * 4) ** -0.5, 0.09375, ((0, 4), (2, 8)))
    router_weight = centred(streams_of[6], (D_MODEL, EXPERTS), D_MODEL ** -0.5, 0.125, ((0, 8), (1, 4)), jnp.float32)
    router_gain = jnp.clip(1.0 + 0.15 * jax.random.normal(streams_of[7], (D_MODEL,), jnp.float32), 0.25, 1.75)
    return {"w_gate": w_gate, "avg_gate": avg_gate, "w_up": w_up, "avg_up": avg_up, "w_down": w_down, "avg_down": avg_down, "router_weight": router_weight, "router_gain": router_gain}


def reference(w_gate, avg_gate, w_up, avg_up, w_down, avg_down, router_weight, router_gain):
    fresh_gate = w_gate + avg_gate.astype(jnp.float32)
    fresh_up = w_up + avg_up.astype(jnp.float32)
    fresh_down = w_down + avg_down.astype(jnp.float32)
    scale_gate = jnp.sqrt(lax.optimization_barrier(jnp.sum(fresh_gate * fresh_gate, axis=1)))
    serve_gate = (fresh_gate / jnp.expand_dims(scale_gate, 1)).astype(jnp.bfloat16)
    scale_up = jnp.sqrt(lax.optimization_barrier(jnp.sum(fresh_up * fresh_up, axis=1)))
    serve_up = (fresh_up / jnp.expand_dims(scale_up, 1)).astype(jnp.bfloat16)
    scale_down = jnp.sqrt(lax.optimization_barrier(jnp.sum(fresh_down * fresh_down, axis=2)))
    serve_down = (fresh_down / jnp.expand_dims(scale_down, 2)).astype(jnp.bfloat16)
    serve_router = (router_weight * router_gain[:, None]).astype(jnp.bfloat16)
    return (serve_gate, serve_up, serve_down, scale_gate, scale_up, scale_down, serve_router)
```

```python
import jax
import jax.numpy as jnp
from jax import lax
from jax.experimental import pallas as pl
from jax.experimental.pallas import tpu as pltpu
from jax.sharding import PartitionSpec as P

LANES = 128
STEP = 4


def columns_sum(w, a, o):
    @pl.loop(0, w.shape[0])
    def _(e):
        fresh = w[e] + a[e].astype(jnp.float32)
        o[e] = jnp.sum(fresh * fresh, axis=0, keepdims=True)


def rows_sum(w, a, o):
    @pl.loop(0, w.shape[0])
    def _(e):
        fresh = w[e] + a[e].astype(jnp.float32)
        square = fresh * fresh
        folded = square[:, :LANES]
        for start in range(LANES, square.shape[1], LANES):
            folded = folded + square[:, start : start + LANES]
        o[e] = jnp.sum(folded.T, axis=0, keepdims=True)


def columns_norm(w, a, s, *refs):
    o = refs[-1]

    @pl.loop(0, w.shape[0])
    def _(e):
        fresh = (w[e] + a[e].astype(jnp.float32)) * (1.0 / s[e])
        for part in range(o.shape[0]):
            o[part, e] = fresh[:, part * LANES : (part + 1) * LANES].astype(o.dtype)


def rows_norm(w, a, s, *refs):
    o = refs[-1]
    height = w.shape[1] // o.shape[0]

    @pl.loop(0, w.shape[0])
    def _(e):
        inverse = 1.0 / s[e]
        for part in range(o.shape[0]):
            rows = slice(part * height, (part + 1) * height)
            factor = jnp.broadcast_to(inverse[:, rows], (LANES, height)).T
            for piece in range(w.shape[2] // LANES):
                lanes = slice(piece * LANES, (piece + 1) * LANES)
                fresh = w[e, rows, lanes] + a[e, rows, lanes].astype(jnp.float32)
                o[part, e, piece * height : (piece + 1) * height, :] = (fresh * factor).astype(o.dtype)


def stack_rows(x, *refs):
    o = refs[-1]
    height = x.shape[2]

    @pl.loop(0, x.shape[1])
    def _(e):
        for part in range(x.shape[0]):
            o[e, part * height : (part + 1) * height, :] = x[part, e]


def stack_columns(x, *refs):
    o = refs[-1]
    height = o.shape[1]
    pieces = x.shape[2] // height

    @pl.loop(0, x.shape[1])
    def _(e):
        for part in range(x.shape[0]):
            for piece in range(pieces):
                start = (part * pieces + piece) * LANES
                o[e, :, start : start + LANES] = x[part, e, piece * height : (piece + 1) * height, :]


def per_expert(shape, first=0):
    return pl.BlockSpec((STEP,) + shape[1:], lambda e: (e + first // STEP, 0, 0))


def per_expert_parts(shape, first=0):
    return pl.BlockSpec((shape[0], STEP) + shape[2:], lambda e: (0, e + first // STEP, 0, 0))


def call(body, count, inputs, specs, out, out_spec, held):
    aliases = {}
    if held is not None:
        aliases = {len(inputs): 0}
        inputs, specs = (*inputs, held), (*specs, pl.BlockSpec(memory_space=pl.ANY))
    moved = int(count * 2**21)
    return pl.pallas_call(
        body,
        grid=(count // STEP,),
        in_specs=list(specs),
        out_specs=out_spec,
        out_shape=out,
        input_output_aliases=aliases,
        cost_estimate=pl.CostEstimate(flops=moved, bytes_accessed=moved, transcendentals=0),
        compiler_params=pltpu.CompilerParams(
            dimension_semantics=("arbitrary",), vmem_limit_bytes=50 * 2**20
        ),
    )(*inputs)


def partial_sums(body, w, a, length, first, count):
    out = jax.ShapeDtypeStruct((count, 1, length), jnp.float32)
    specs = (per_expert(w.shape, first), per_expert(a.shape, first))
    return call(body, count, (w, a), specs, out, per_expert(out.shape), None)


def normalised(body, w, a, first, scale, scale_first, count, shape, slot=0, held=None):
    out = jax.ShapeDtypeStruct(shape, jnp.bfloat16)
    specs = (per_expert(w.shape, first), per_expert(a.shape, first), per_expert(scale.shape, scale_first))
    return call(body, count, (w, a, scale), specs, out, per_expert_parts(shape, slot), held)


def placed(body, x, slot, count, shape, first=0, held=None):
    out = jax.ShapeDtypeStruct(shape, jnp.bfloat16)
    return call(body, count, (x,), (per_expert_parts(x.shape, slot),), out, per_expert(shape, first), held)


def exchanged(x):
    return lax.all_to_all(x, "rows", split_axis=0, concat_axis=0, tiled=True)


def shards(parts, w_gate, avg_gate, w_up, avg_up, w_down, avg_down, router_weight, router_gain):
    experts, high, wide = w_gate.shape
    tall, deep = w_down.shape[1:]
    block, slab = wide // parts, tall // parts
    rank = lax.axis_index("rows")
    early = experts * 3 // 4 // STEP * STEP
    late = experts // 2 // STEP * STEP
    kept = experts - early

    part_router = (router_weight * router_gain[:, None]).astype(jnp.bfloat16).astype(jnp.float32).T
    columns, rows = part_router.shape
    head = partial_sums(columns_sum, w_gate, avg_gate, wide, 0, early)
    gathered = lax.all_gather(
        jnp.concatenate((head, part_router.reshape(-1, 1, wide))), "rows"
    )
    scale_head = jnp.sqrt(jnp.sum(gathered[:, :early], axis=0))
    row_router = gathered[:, early:].reshape(parts, columns, rows)

    send_a = normalised(
        columns_norm, w_gate, avg_gate, 0, scale_head, 0, early, (parts, early, high, block)
    )
    send_a, w_up, avg_up, w_down, avg_down, w_gate, avg_gate = lax.optimization_barrier(
        (send_a, w_up, avg_up, w_down, avg_down, w_gate, avg_gate)
    )
    got_a = exchanged(send_a)

    part_rest = partial_sums(columns_sum, w_gate, avg_gate, wide, early, kept)
    part_up = partial_sums(columns_sum, w_up, avg_up, wide, 0, experts)
    part_down = partial_sums(rows_sum, w_down, avg_down, tall, 0, experts)
    total_columns, total_down = lax.psum(
        (jnp.concatenate((part_up, part_rest)), part_down), "rows"
    )
    scale_columns, scale_down = jnp.sqrt(total_columns), jnp.sqrt(total_down)
    scale_up, scale_rest = scale_columns[:experts], scale_columns[experts:]
    shape_b = (parts, kept + experts + late, high, block)
    send_b = normalised(columns_norm, w_gate, avg_gate, early, scale_columns, experts, kept, shape_b)
    send_b = normalised(columns_norm, w_up, avg_up, 0, scale_columns, 0, experts, shape_b, kept, send_b)
    send_b = normalised(
        rows_norm, w_down, avg_down, 0, scale_down, 0, late, shape_b, kept + experts, send_b
    )
    send_b, scale_last = lax.optimization_barrier((send_b, scale_down))
    got_b = exchanged(send_b)

    last = experts - late
    send_c = normalised(
        rows_norm, w_down, avg_down, late, scale_last, late, last, (parts, last, high, block)
    )
    shape_columns = (experts, high * parts, block)
    shape_down = (experts, slab, deep * parts)
    serve_gate = placed(stack_rows, got_a, 0, early, shape_columns)
    row_router, send_c = lax.optimization_barrier((row_router, send_c))
    got_c = exchanged(send_c)
    row_router = row_router.transpose(1, 0, 2).reshape(columns, parts * rows).astype(jnp.bfloat16)
    serve_router = lax.all_gather(row_router, "owner", axis=0, tiled=True).T

    serve_gate = placed(stack_rows, got_b, 0, kept, shape_columns, early, serve_gate)
    serve_up = placed(stack_rows, got_b, kept, experts, shape_columns)
    serve_down = placed(stack_columns, got_b, kept + experts, late, shape_down)
    serve_down = placed(stack_columns, got_c, 0, last, shape_down, late, serve_down)

    def own(scale, width):
        return lax.dynamic_slice_in_dim(scale[:, 0, :], rank * width, width, axis=1)

    return (
        serve_gate,
        serve_up,
        serve_down,
        own(jnp.concatenate((scale_head, scale_rest)), block),
        own(scale_up, block),
        own(scale_down, slab),
        serve_router,
    )


def plain_shards(w_gate, avg_gate, w_up, avg_up, w_down, avg_down, router_weight, router_gain):
    def served(w, a, axis, split):
        fresh = w + a.astype(jnp.float32)
        scale = jnp.sqrt(lax.psum(jnp.sum(fresh * fresh, axis=axis), "rows"))
        narrow = (fresh / jnp.expand_dims(scale, axis)).astype(jnp.bfloat16)
        serve = lax.all_to_all(narrow, "rows", split_axis=split, concat_axis=axis, tiled=True)
        width = serve.shape[split]
        return serve, lax.dynamic_slice_in_dim(scale, lax.axis_index("rows") * width, width, axis=1)

    serve_gate, scale_gate = served(w_gate, avg_gate, 1, 2)
    serve_up, scale_up = served(w_up, avg_up, 1, 2)
    serve_down, scale_down = served(w_down, avg_down, 2, 1)
    part_router = (router_weight * router_gain[:, None]).astype(jnp.bfloat16)
    row_router = lax.all_gather(part_router, "rows", axis=0, tiled=True)
    serve_router = lax.all_gather(row_router, "owner", axis=1, tiled=True)
    return (serve_gate, serve_up, serve_down, scale_gate, scale_up, scale_down, serve_router)


def solution(mesh):
    parts = mesh.shape["rows"]

    def dispatched(*args):
        experts, high, wide = args[0].shape
        tall, deep = args[4].shape[1:]
        block, slab = wide // parts, tall // parts
        aligned = block == LANES and slab % LANES == 0 and deep % LANES == 0
        aligned = aligned and slab * deep == high * block and experts % STEP == 0
        aligned = aligned and experts >= 2 * STEP and args[6].size % wide == 0
        return shards(parts, *args) if aligned else plain_shards(*args)

    return jax.shard_map(
        dispatched,
        mesh=mesh,
        in_specs=(
            P("owner", "rows", None),
            P("owner", "rows", None),
            P("owner", "rows", None),
            P("owner", "rows", None),
            P("owner", None, "rows"),
            P("owner", None, "rows"),
            P("rows", "owner"),
            P("rows"),
        ),
        out_specs=(
            P("owner", None, "rows"),
            P("owner", None, "rows"),
            P("owner", "rows", None),
            P("owner", "rows"),
            P("owner", "rows"),
            P("owner", "rows"),
            P(),
        ),
        check_vma=False,
    )
```
